32 devices in a mesh: row: 16 (over z, y, core), col: 2 (over x).
Axes of the slice: x: 2, y: 2, z: 4, core: 2. Of those that a mesh axis runs over, the one named last changes fastest.
Arguments:
- kernel: float32 [5120, 65536], P('row', 'col'), may hold values from -0.0234375 to 0.0234375
- slip: float32 [512, 65536], P('row', 'col'), may hold values from -6 to 6
- segment: int32 [5120], P(('row', 'col')), may hold values from 0 to 15
- prestress: float32 [5120, 512], P(('row', 'col')), may hold values from -4 to 4
- state: float32 [5120, 512], P(('row', 'col')), may hold values from 0.5 to 2
- normal_stress: float32 [5120], P(('row', 'col')), may hold values from 2 to 8
- a_table: float32 [16], replicated, may hold values from 0.5 to 1
- b_table: float32 [16], replicated, may hold values from 0.5 to 1
Outputs:
- new_rate: float32 [5120, 512], P(('row', 'col'))
- new_state: float32 [5120, 512], P(('row', 'col'))
The draws below stay inside these ranges and needn't reach their ends.
All inputs are finite; a program needn't handle non-finite values.
Results may differ from the reference program's by a relative error of at most 0.00016.
Values sent between devices are 32-bit elements; how exact they have to be, the bound alone decides.
A program may use at most 192 MiB of HBM per device.

```python
import math
import jax
import jax.numpy as jnp
from jax import lax

N = 65536
MEMBERS = 512
SEGS = 16
M = 5120


def place_ends(drawn, key, smallest, high):
    place = [jax.random.randint(jax.random.fold_in(key, axis), (), 0, length) for axis, length in enumerate(drawn.shape)]
    widest = drawn.shape.index(max(drawn.shape))
    beside = place[:widest] + [(place[widest] + 1) % drawn.shape[widest]] + place[widest + 1:]
    return drawn.at[tuple(place)].set(smallest).at[tuple(beside)].set(high)


def block_levels(rng, dims, shards, smallest, top_value):
    def one(axis_at, blocks):
        steps = jax.random.uniform(jax.random.fold_in(jax.random.fold_in(rng, 6), axis_at), (blocks,), jnp.float32, smallest / len(shards), top_value / len(shards))
        return jnp.repeat(jnp.exp(steps), dims[axis_at] // blocks).reshape((-1,) + (1,) * (len(dims) - axis_at - 1))

    gain = one(*shards[0])
    for cut in shards[1:]:
        gain = gain * one(*cut)
    return gain


def gaussian(own_key, extent, scale, limit, cuts=(), held_as=jnp.bfloat16):
    values = jax.random.normal(own_key, extent, jnp.float32) * scale
    if len(cuts) > 0:
        values = block_levels(own_key, extent, cuts, -0.22, 0.18) * values
    return jnp.clip(values, min=-limit, max=limit).astype(held_as)


def setup_inputs(seed: int = 0) -> dict:
    seeds = jax.random.split(jax.random.key(seed), 9)
    return {
        "kernel": gaussian(seeds[0], (M, N), N ** -0.5, 0.0234375, ((0, 16), (1, 2)), jnp.float32),
        "slip": gaussian(seeds[1], (MEMBERS, N), 1.0, 6.0, ((0, 16), (1, 2)), jnp.float32),
        "segment": place_ends(jax.random.randint(seeds[2], (M,), 0, SEGS), jax.random.fold_in(seeds[2], 1), 0, SEGS - 1).astype(jnp.int32),
        "prestress": gaussian(seeds[3], (M, MEMBERS), 0.5, 4.0, ((0, 32),), jnp.float32),
        "state": jnp.clip(jnp.exp(math.log(2.0) - 1.3862944 * jax.random.uniform(seeds[4], (M, MEMBERS), jnp.float32) ** block_levels(seeds[4], (M, MEMBERS), ((0, 32),), -0.2, 0.2)), 0.5, 2.0),
        "normal_stress": jnp.clip(jnp.exp(math.log(8.0) - 1.3862944 * jax.random.uniform(seeds[5], (M,), jnp.float32) ** block_levels(seeds[5], (M,), ((0, 32),), -0.2, 0.2)), 2.0, 8.0),
        "a_table": jnp.clip(jnp.exp(jax.random.uniform(seeds[6], (SEGS,), jnp.float32, math.log(0.5), math.log(1.0))), 0.5, 1.0),
        "b_table": jnp.clip(jnp.exp(jax.random.uniform(seeds[7], (SEGS,), jnp.float32, math.log(0.5), math.log(1.0))), 0.5, 1.0),
    }


def reference(kernel, slip, segment, prestress, state, normal_stress, a_table, b_table):
    traction = lax.dot_general(kernel, slip, (((1,), (1,)), ((), ())), precision=lax.Precision.HIGHEST, preferred_element_type=jnp.float32)
    onehot = (segment[:, None] == jnp.arange(SEGS, dtype=jnp.int32)[None, :]).astype(jnp.float32)
    a_rows = jnp.dot(onehot, a_table, precision=lax.Precision.HIGHEST)
    b_rows = jnp.dot(onehot, b_table, precision=lax.Precision.HIGHEST)
    stress = prestress + traction
    new_rate = jnp.exp(-(b_rows / a_rows)[:, None] * jnp.log(state)) * jnp.sinh(stress / (a_rows * normal_stress)[:, None])
    new_state = state + 0.1 * (1.0 - new_rate * state)
    return new_rate, new_state
```

```python
import functools

import jax
import jax.numpy as jnp
from jax import lax
from jax.experimental import pallas as pl
from jax.experimental.pallas import tpu as pltpu
from jax.sharding import PartitionSpec as P

CHUNKS = 16
MESH = pl.DeviceIdType.MESH


def split(value):
    high = value.astype(jnp.bfloat16)
    return high, (value - high.astype(jnp.float32)).astype(jnp.bfloat16)


def times(left, right):
    return lax.dot_general(
        left, right, (((1,), (1,)), ((), ())), preferred_element_type=jnp.float32
    )


def gather_product(
    rows, kernel_ref, slip_ref, total, held, slip_in, kernel_in,
    ring_send, ring_recv, pair_send, pair_recv, own_send, own_recv, slip_sem, kernel_sem,
):
    members = slip_ref.shape[0]
    width = slip_ref.shape[1] // CHUNKS
    chips = rows // 2
    rounds = chips - 1
    pairs = CHUNKS // 2
    me = lax.axis_index("row")
    core = lax.rem(me, 2)
    other = me + 1 - 2 * core
    chip = me // 2
    odd = chip % 2
    place = (1 - odd) * (chip // 2) + odd * (chips - 1 - chip // 2)

    def row_at(spot, which):
        spot = (spot + chips) % chips
        back = spot // (chips // 2)
        return ((1 - back) * 2 * spot + back * (2 * (chips - 1 - spot) + 1)) * 2 + which

    def block(ref, row, chunk):
        return ref.at[
            pl.ds(pl.multiple_of(row * members, members), members),
            pl.ds(pl.multiple_of(chunk * width, width), width),
        ]

    def own(chunk):
        return slip_ref.at[:, pl.ds(pl.multiple_of(chunk * width, width), width)]

    def chunk_of(pair, way, step):
        return 2 * pair + (step + way) % 2

    def origin(way, hops):
        return place - hops if way == 0 else place + hops

    def ring(pair, way, step):
        chunk = chunk_of(pair, way, step)
        hops = step // 2
        row = row_at(origin(way, hops), core)
        return pltpu.make_async_remote_copy(
            src_ref=own(chunk) if hops == 0 else block(held, row, chunk),
            dst_ref=block(held, row, chunk),
            send_sem=ring_send.at[way, step],
            recv_sem=ring_recv.at[pair % 2, way, step],
            device_id={"row": row_at(place + 1 if way == 0 else place - 1, core)},
            device_id_type=MESH,
        )

    def across(pair, way, step):
        chunk = chunk_of(pair, way, step)
        piece = block(held, row_at(origin(way, step // 2 + 1), core), chunk)
        return pltpu.make_async_remote_copy(
            src_ref=piece,
            dst_ref=piece,
            send_sem=pair_send.at[way, step],
            recv_sem=pair_recv.at[pair % 3, way, step],
            device_id={"row": other},
            device_id_type=MESH,
        )

    def across_own(pair, side):
        chunk = 2 * pair + side
        return pltpu.make_async_remote_copy(
            src_ref=own(chunk),
            dst_ref=block(held, me, chunk),
            send_sem=own_send.at[side],
            recv_sem=own_recv.at[pair % 3, side],
            device_id={"row": other},
            device_id_type=MESH,
        )

    def kernel_load(chunk, side):
        return pltpu.make_async_copy(
            kernel_ref.at[:, pl.ds(pl.multiple_of(chunk * width, width), width)],
            kernel_in.at[side],
            kernel_sem.at[side],
        )

    def slip_start(chunk, side):
        def place_in(row):
            return slip_in.at[side, pl.ds(pl.multiple_of(row * members, members), members)]

        pltpu.make_async_copy(own(chunk), place_in(me), slip_sem.at[side]).start()

        def one(at, carry):
            row = (me + at) % rows
            pltpu.make_async_copy(
                block(held, row, chunk), place_in(row), slip_sem.at[side]
            ).start()
            return carry

        lax.fori_loop(1, rows, one, 0)

    def slip_wait(chunk, side):
        pltpu.make_async_copy(
            held.at[:, pl.ds(pl.multiple_of(chunk * width, width), width)],
            slip_in.at[side],
            slip_sem.at[side],
        ).wait()

    depth = min(width, 512)

    def product(side):
        def one(at, carry):
            columns = pl.ds(pl.multiple_of(at * depth, depth), depth)
            k_high, k_low = split(kernel_in[side, :, columns])
            s_high, s_low = split(slip_in[side, :, columns])
            total[...] += times(k_high, s_high) + (times(k_high, s_low) + times(k_low, s_high))
            return carry

        lax.fori_loop(0, width // depth, one, 0)

    total[...] = jnp.zeros_like(total)

    def arrival(pair, way, step):
        ring(pair, way, step).wait_recv()

    def pass_across(pair, way, step):
        @pl.when(pair > 0)
        def _():
            across(pair, way, step).wait_send()

        across(pair, way, step).start()

    def travel(pair, carry):
        sending = pair < pairs
        draining = pair > 0
        for step in range(rounds):

            @pl.when(sending)
            def _():
                for way in range(2):
                    if step >= 2:
                        arrival(pair, way, step - 2)

                    @pl.when(draining)
                    def _():
                        ring(pair, way, step).wait_send()

                    ring(pair, way, step).start()
                if step < 2:

                    @pl.when(draining)
                    def _():
                        across_own(pair, step).wait_send()

                    across_own(pair, step).start()
                else:
                    for way in range(2):
                        pass_across(pair, way, step - 2)

            @pl.when(draining)
            def _():
                if step < 2:
                    for way in range(2):
                        arrival(pair - 1, way, rounds - 2 + step)
                        pass_across(pair - 1, way, rounds - 2 + step)
                if step == 0:
                    for side in range(2):
                        kernel_load(2 * pair - 2 + side, side).start()
                if step == 2:
                    for side in range(2):
                        across_own(pair - 1, side).wait_recv()
                    for way in range(2):
                        for back in range(rounds):
                            across(pair - 1, way, back).wait_recv()
                    for side in range(2):
                        slip_start(2 * pair - 2 + side, side)
                if step in (3, 5):
                    side = (step - 3) // 2
                    kernel_load(2 * pair - 2 + side, side).wait()
                    slip_wait(2 * pair - 2 + side, side)
                    product(side)

        return carry

    lax.fori_loop(0, pairs + 1, travel, 0)
    last = pairs - 1
    for way in range(2):
        for step in range(rounds):
            ring(last, way, step).wait_send()
            across(last, way, step).wait_send()
    for side in range(2):
        across_own(last, side).wait_send()


def traction_partial(rows, kernel, slip):
    targets, columns = kernel.shape
    members = slip.shape[0] * rows
    width = columns // CHUNKS
    rounds = rows // 2 - 1
    dma = pltpu.SemaphoreType.DMA
    flops = 6 * targets * members * columns
    return pl.pallas_call(
        functools.partial(gather_product, rows),
        out_shape=(
            jax.ShapeDtypeStruct((targets, members), jnp.float32),
            jax.ShapeDtypeStruct((members, columns), jnp.float32),
        ),
        in_specs=[pl.BlockSpec(memory_space=pl.ANY)] * 2,
        out_specs=(pl.BlockSpec(memory_space=pltpu.VMEM), pl.BlockSpec(memory_space=pl.ANY)),
        scratch_shapes=[
            pltpu.VMEM((2, members, width), jnp.float32),
            pltpu.VMEM((2, targets, width), jnp.float32),
            dma((2, rounds)),
            dma((2, 2, rounds)),
            dma((2, rounds)),
            dma((3, 2, rounds)),
            dma((2,)),
            dma((3, 2)),
            dma((2,)),
            dma((2,)),
        ],
        compiler_params=pltpu.CompilerParams(
            has_side_effects=True, vmem_limit_bytes=48 * 1024 * 1024
        ),
        cost_estimate=pl.CostEstimate(
            flops=flops, bytes_accessed=4 * members * columns * 4, transcendentals=0
        ),
    )(kernel, slip)[0]


def add_over_columns(partial_value, columns):
    if columns != 2:
        return lax.psum_scatter(partial_value, "col", scatter_dimension=0, tiled=True)
    half = partial_value.shape[0] // 2
    me = lax.axis_index("col")
    mine = lax.dynamic_slice_in_dim(partial_value, me * half, half, 0)
    theirs = lax.dynamic_slice_in_dim(partial_value, (1 - me) * half, half, 0)
    return mine + lax.ppermute(theirs, "col", [(0, 1), (1, 0)])


def friction(traction, segment, prestress, state, normal_stress, a_table, b_table):
    onehot = (segment[:, None] == jnp.arange(a_table.shape[0], dtype=jnp.int32)[None, :]).astype(
        jnp.float32
    )
    a_rows = jnp.dot(onehot, a_table, precision=lax.Precision.HIGHEST)
    b_rows = jnp.dot(onehot, b_table, precision=lax.Precision.HIGHEST)
    stress = prestress + traction
    new_rate = jnp.exp(-(b_rows / a_rows)[:, None] * jnp.log(state)) * jnp.sinh(
        stress / (a_rows * normal_stress)[:, None]
    )
    new_state = state + 0.1 * (1.0 - new_rate * state)
    return (new_rate, new_state)


def per_device(rows, columns, kernel, slip, segment, prestress, state, normal_stress, a_table, b_table):
    traction = add_over_columns(traction_partial(rows, kernel, slip), columns)
    return friction(traction, segment, prestress, state, normal_stress, a_table, b_table)


def solution(mesh):
    placed = (
        P("row", "col"),
        P("row", "col"),
        P(("row", "col")),
        P(("row", "col"), None),
        P(("row", "col"), None),
        P(("row", "col")),
        P(),
        P(),
    )
    return jax.shard_map(
        functools.partial(per_device, mesh.shape["row"], mesh.shape["col"]),
        mesh=mesh,
        in_specs=placed,
        out_specs=(P(("row", "col"), None), P(("row", "col"), None)),
        check_vma=False,
    )
```
